32 devices in a mesh: row: 8 (over z, core), col: 4 (over y, x).
Axes of the slice: x: 2, y: 2, z: 4, core: 2. Of those that a mesh axis runs over, the one named last changes fastest.
Arguments:
- loadings: bfloat16 [8, 32768, 1024], P(None, 'row', 'col'), may hold values from -6 to 6
- weights: bfloat16 [8, 32768, 512], P(None, 'row', 'col'), may hold values from -0.03125 to 0.03125
- specific: float32 [8, 32768], P(None, 'row'), may hold values from 0.2 to 5
- factor_cov: float32 [8, 1024, 1024], P(None, 'col'), may hold values from -0.001953125 to 0.0048828125, as said below
Outputs:
- portfolio_cov: float32 [8, 512, 512], P(None, 'row', 'col')
The draws below stay inside these ranges and needn't reach their ends.
Inputs may be any that keep to these rules, and one draw needn't show every extreme that they name: `factor_cov`: each day's matrix is a symmetric positive definite factor covariance of order 1024.
All inputs are finite; a program needn't handle non-finite values.
Results may differ from the reference program's by a relative error of at most 0.0003.
Values may be sent and summed in bfloat16 or wider, within the bound.
A program may use at most 128 MiB of HBM per device.

```python
import math
import jax
import jax.numpy as jnp
from jax import lax

N = 32768
R = 1024
K = 512
DAYS = 8


def draw_factor_cov(key, part):
    first_key, second_key = jax.random.split(jax.random.fold_in(key, 11))
    noise = jax.random.normal(first_key, (DAYS, R, R), jnp.float32)
    symmetric = (noise + jnp.swapaxes(noise, 1, 2)) / jnp.sqrt(2.0 * R)
    variances = jax.random.uniform(second_key, (DAYS, R), jnp.float32, 1.0, 3.0)
    identity = jnp.eye(R, dtype=jnp.float32)
    return (identity[None, :, :] * variances[:, :, None] + 0.4 * symmetric) / R


def steps_of(rng, extent, pieces, smallest, largest):
    loudness, own = 1.0, jax.random.fold_in(rng, 6)
    for position, parts in pieces:
        steps = jnp.exp(jax.random.uniform(jax.random.fold_in(own, position), (parts,), jnp.float32, smallest / len(pieces), largest / len(pieces)))
        loudness = loudness * jnp.repeat(steps, extent[position] // parts).reshape([-1 if axis == position else 1 for axis in range(len(extent))])
    return loudness


def normal_values(rng, dims, spread, reach, cuts=(), kind=jnp.bfloat16):
    result = spread * jax.random.normal(rng, dims, jnp.float32)
    if cuts:
        result = result * steps_of(rng, dims, cuts, -0.22, 0.18)
    return jnp.clip(result, -reach, reach).astype(kind)


def setup_inputs(seed: int = 0) -> dict:
    keys = jax.random.split(jax.random.key(seed), 5)
    return {
        "loadings": normal_values(keys[0], (DAYS, N, R), 1.0, 6.0, ((1, 8), (2, 4))),
        "weights": normal_values(keys[1], (DAYS, N, K), N ** -0.5, 0.03125, ((1, 8), (2, 4))),
        "specific": jnp.clip(jnp.exp(math.log(5.0) - 3.218876 * jax.random.uniform(keys[2], (DAYS, N), jnp.float32) ** steps_of(keys[2], (DAYS, N), ((1, 8),), -0.2, 0.2)), 0.2, 5.0),
        "factor_cov": draw_factor_cov(jax.random.fold_in(keys[4], 71), 0),
    }


def one_day(operands):
    loadings, weights, specific, factor_cov = operands
    exposure = jnp.dot(loadings.T, weights, preferred_element_type=jnp.float32)
    weighted = (specific[:, None] * weights.astype(jnp.float32)).astype(jnp.bfloat16)
    specific_cov = jnp.dot(weights.T, weighted, preferred_element_type=jnp.float32)
    left = jnp.dot(exposure.T, factor_cov, precision=lax.Precision.HIGHEST)
    return jnp.dot(left, exposure, precision=lax.Precision.HIGHEST) + specific_cov


def reference(loadings, weights, specific, factor_cov):
    return lax.map(one_day, (loadings, weights, specific, factor_cov))
```

```python
import functools

import jax
import jax.numpy as jnp
from jax import lax
from jax.experimental import pallas as pl
from jax.experimental.pallas import tpu as pltpu
from jax.sharding import PartitionSpec as P

F32, BF16 = jnp.float32, jnp.bfloat16
HIGHEST = lax.Precision.HIGHEST
CUTS, AHEAD, EXTRA = 4, 2, 1
LAGS = (4, 5, 5, 6, 9, 11, 13, 16, 19)
GIVEN = (((0, 0), (0, 1), (0, 2)), ((0, 3), (1, 0)), ((1, 1),), ((1, 2), (1, 3)))


def by_dim(a, b, dim, precision=None):
    return lax.dot_general(
        a, b, (((dim,), (dim,)), ((), ())), precision=precision, preferred_element_type=F32
    )


def kernel(
    rows, cols, cuts, load_hbm, weight_hbm, spec_ref, fcov_hbm, out_ref,
    held, load, load_in, fcov, weighted, part, mate_in, pair, part_in, swap, swap_in,
    exp_rows, exp_cols, own_spec, prod, prod_in,
    w_sem, l_sem, f_sem, g_send, g_recv, m_send, m_recv, p_send, p_recv, s_send, s_recv,
    er_send, er_recv, ec_send, ec_recv, q_send, q_recv,
):
    days, assets, factors = load_hbm.shape
    ports = weight_hbm.shape[2]
    slab = ports * cols // rows
    row, col = lax.axis_index("row"), lax.axis_index("col")
    near_x = col + 1 - 2 * (col % 2)
    near_y = (col + 2) % 4
    far = 3 - col
    chips, per = rows // 2, rows // cols
    half = assets // 2
    piece = half // cuts
    mine, core = row // 2, row % 2
    spans = (pl.ds(0, factors), pl.ds(factors, factors), pl.ds(2 * factors, 2 * ports))
    mate = row + 1 - 2 * core

    def merger(d):
        return near_x + (d % 2) * (near_y - near_x)

    def other(d):
        return near_y + (d % 2) * (near_x - near_y)

    def side(d):
        return col % 2 + (d % 2) * (col // 2 - col % 2)

    def to_row(r):
        return {"row": r, "col": col}

    def to_col(c):
        return {"row": row, "col": c}

    def remote(src, dst, send, recv, where):
        return pltpu.make_async_remote_copy(
            src_ref=src, dst_ref=dst, send_sem=send, recv_sem=recv,
            device_id=where, device_id_type=pl.DeviceIdType.MESH,
        )

    def kept(d, start, size):
        return pl.ds(pl.multiple_of(side(d) * half + start, piece), size)

    def given(d, start, size):
        return pl.ds(pl.multiple_of((1 - side(d)) * half + start, piece), size)

    def gather(u, lane, block):
        d, start = u // cuts, pl.multiple_of((u % cuts) * piece, piece)
        if lane == 1:
            dst = load_in.at[d, pl.ds(start, piece)]
            src = load_hbm.at[d, given(d, start, piece)]
        else:
            dst = held.at[d, block, pl.ds(start, piece)]
            src = dst
        if lane == 0:
            src = weight_hbm.at[d, given(d, start, piece)]
        if lane == 2:
            src = weight_hbm.at[d, kept(d, start, piece)]
        where = merger(d) if lane < 2 else other(d)
        return remote(src, dst, g_send.at[u, lane], g_recv.at[u, lane], to_col(where))

    def own_weights(d):
        return pltpu.make_async_copy(
            weight_hbm.at[d, kept(d, 0, half)], held.at[d, col], w_sem.at[d]
        )

    def get_load(d):
        return pltpu.make_async_copy(
            load_hbm.at[d, kept(d, 0, half)], load.at[d % 2], l_sem.at[d % 2]
        )

    def get_fcov(d):
        return pltpu.make_async_copy(fcov_hbm.at[d], fcov.at[d % 2], f_sem.at[d % 2])

    def mate_copy(d, lane):
        span = spans[lane]
        return remote(
            part.at[d % 2, 1 - core, :, :, span], mate_in.at[d, :, :, span],
            m_send.at[d, lane], m_recv.at[d, lane], to_row(mate),
        )

    def part_copy(d, lane, other_chip, landed):
        span = spans[lane]
        return remote(
            pair.at[d % 2, other_chip, :, span], part_in.at[d, landed, :, span],
            p_send.at[d, lane, other_chip], p_recv.at[d, lane, landed],
            to_row(2 * other_chip + core),
        )

    def summed(d, lane):
        for peer in chip_peers():
            part_copy(d, lane, mine, peer).wait_recv()
        total = part_in[d, 0, :, spans[lane]]
        for z in range(1, chips):
            total = total + part_in[d, z, :, spans[lane]]
        return total

    def swap_copy(d):
        return remote(
            swap.at[d], swap_in.at[d], s_send.at[d], s_recv.at[d], to_col(merger(d))
        )

    def exp_gather(d, lane, block):
        start, size = (slab // 2 if lane == 3 else 0), (slab if lane < 2 else slab // 2)
        ref = exp_cols.at[d, block, pl.ds(start, size)]
        where = near_x if lane in (0, 3) else near_y
        return remote(ref, ref, ec_send.at[d, lane], ec_recv.at[d, lane], to_col(where))

    def exp_row_copy(d, slot, landed, other_row):
        ref = exp_rows.at[d, pl.ds(pl.multiple_of(landed * slab, slab), slab)]
        return remote(ref, ref, er_send.at[d, slot], er_recv.at[d, landed], to_row(other_row))

    def prod_copy(d, other_col, landed):
        return remote(
            prod.at[d, other_col], prod_in.at[d, landed],
            q_send.at[d, other_col], q_recv.at[d, landed], to_col(other_col),
        )

    def row_peers():
        return [(row + step) % rows for step in range(1, rows)]

    def chip_peers():
        return [(mine + step) % chips for step in range(1, chips)]

    def col_peers():
        return [near_x, near_y, far]

    def exchange_own(u):
        gather(u, 2, col).start()

    def donate(u):
        first = u - u % cuts
        for q, parts in enumerate(GIVEN):
            @pl.when(u % cuts == q)
            def _(parts=parts):
                for lane, part_of_day in parts:
                    gather(first + part_of_day, lane, col).start()

    def pass_on(u):
        block = merger(u // cuts)

        @pl.when(u % cuts < cuts // 2)
        def _():
            for step in range(2):
                chunk = u + u % cuts + step
                gather(chunk, 0, block).wait_recv()
                gather(chunk, 3, block).start()

    def store(slot, j, lane, values):
        for i in range(per):
            place = j * (per // 2) + i // 2
            part[slot, i % 2, place, :, pl.ds(lane, values.shape[1])] = (
                values[i * slab : (i + 1) * slab]
            )

    def sum_own(d, j):
        slot = d % 2
        lhs = held[d, j]
        store(slot, j, factors, by_dim(lhs, load[slot], 0))
        store(slot, j, 2 * factors, by_dim(lhs, weighted[...], 0))

    def own_sums(d):
        for q in range(cuts):
            gather(d * cuts + q, 2, other(d)).wait_recv()
            gather(d * cuts + q, 3, far).wait_recv()
        own_weights(d).wait()
        groups = half // 128
        scales = spec_ref[d, pl.ds(pl.multiple_of(side(d) * groups, groups), groups)]
        copies = -(-128 // groups)
        tall = jnp.concatenate([scales] * copies, axis=0).T
        for i in range(groups):
            span = pl.ds(i * 128, 128)
            for lane, block in enumerate((col, merger(d))):
                scaled = held[d, block, span].astype(F32) * tall[:, i : i + 1]
                weighted[span, pl.ds(lane * ports, ports)] = scaled.astype(BF16)

        @pl.when(d >= 2)
        def _():
            for lane in range(3):
                mate_copy(d - 2, lane).wait_send()
                for peer in chip_peers():
                    part_copy(d - 2, lane, peer, mine).wait_send()

        get_load(d).wait()

        def own_block(j, carry):
            sum_own(d, j)
            return carry

        lax.fori_loop(0, cols, own_block, 0)
        mate_copy(d, 1).start()
        mate_copy(d, 2).start()

        @pl.when(d + 2 < days)
        def _():
            get_load(d + 2).start()

    def merged_sums(d):
        for q in range(cuts):
            gather(d * cuts + q, 1, col).wait_recv()

        def merged_block(j, carry):
            store(d % 2, j, 0, by_dim(held[d, j], load_in[d], 0))
            return carry

        lax.fori_loop(0, cols, merged_block, 0)
        mate_copy(d, 0).start()

    def pair_up(d, lane):
        slot, span = d % 2, spans[lane]
        mate_copy(d, lane).wait_recv()
        for peer in chip_peers():
            pair[slot, peer, :, span] = part[slot, core, peer, :, span] + mate_in[d, peer, :, span]
            part_copy(d, lane, peer, mine).start()
        part_in[d, mine, :, span] = part[slot, core, mine, :, span] + mate_in[d, mine, :, span]

    def pair_own(d):
        pair_up(d, 1)

    def pair_merged(d):
        pair_up(d, 0)

    def trade(d):
        swap[d] = summed(d, 0)
        swap_copy(d).start()

    def exposures(d):
        total = summed(d, 1)
        swap_copy(d).wait_recv()
        own = total + swap_in[d]
        exp_cols[d, col] = own
        exp_rows[d, pl.ds(pl.multiple_of(row * slab, slab), slab)] = own
        for peer in chip_peers():
            exp_row_copy(d, 2 * peer + core, row, 2 * peer + core).start()
        exp_gather(d, 0, col).start()
        exp_gather(d, 1, col).start()
        exp_row_copy(d, mate, row, mate).start()
        pair_up(d, 2)

    def share(d):
        exp_gather(d, 0, near_x).wait_recv()
        exp_gather(d, 2, near_x).start()
        exp_gather(d, 1, near_y).wait_recv()
        exp_gather(d, 3, near_y).start()
        for peer in chip_peers():
            exp_row_copy(d, row, 2 * peer + core, mate).wait_recv()
            exp_row_copy(d, 2 * peer + 1 - core, 2 * peer + core, mate).start()

    def products(d):
        slot = d % 2
        get_fcov(d).wait()
        exp_gather(d, 2, far).wait_recv()
        exp_gather(d, 3, far).wait_recv()
        left = jnp.zeros((slab, factors), F32)
        for j in range(cols):
            left = left + by_dim(
                exp_cols[d, j], fcov[slot, :, pl.ds(j * factors, factors)], 1, HIGHEST
            )

        @pl.when(d + 2 < days)
        def _():
            get_fcov(d + 2).start()

        exp_row_copy(d, row, mate, mate).wait_recv()
        for peer in chip_peers():
            exp_row_copy(d, row, 2 * peer + 1 - core, mate).wait_recv()
        for j in range(cols):
            prod[d, j] = by_dim(left, exp_rows[d, pl.ds(j * ports, ports)], 1, HIGHEST)
        block = merger(d)
        total = summed(d, 2)
        own_spec[d] = total[:, :ports]
        prod[d, block] = prod[d, block] + total[:, ports:]
        for peer in col_peers():
            prod_copy(d, peer, col).start()
        prod_in[d, col] = prod[d, col]

    def finish(d):
        for peer in col_peers():
            prod_copy(d, col, peer).wait_recv()
        total = own_spec[d]
        for j in range(cols):
            total = total + prod_in[d, j]
        out_ref[d] = total

    barrier = pltpu.get_barrier_semaphore()
    for peer in row_peers():
        pl.semaphore_signal(
            barrier, inc=1, device_id=to_row(peer), device_id_type=pl.DeviceIdType.MESH
        )
    for peer in col_peers():
        pl.semaphore_signal(
            barrier, inc=1, device_id=to_col(peer), device_id_type=pl.DeviceIdType.MESH
        )
    for d in range(days):
        own_weights(d).start()
    for d in range(min(2, days)):
        get_load(d).start()
        get_fcov(d).start()
    pl.semaphore_wait(barrier, rows + cols - 2)

    units = cuts * days
    for u in range(AHEAD):
        exchange_own(u)
    for u in range(AHEAD + EXTRA):
        if u < AHEAD or (u // cuts) % 2 == 1:
            donate(u)

    def turn(t, carry):
        def stage(lag, what):
            @pl.when((t >= lag) & ((t - lag) % cuts == 0) & (t - lag < units))
            def _():
                what((t - lag) // cuts)

        soon, later = t + AHEAD, t + AHEAD + EXTRA

        @pl.when((soon < units) & ((soon // cuts) % 2 == 0))
        def _():
            donate(soon)

        @pl.when(soon < units)
        def _():
            exchange_own(soon)

        @pl.when((later < units) & ((later // cuts) % 2 == 1))
        def _():
            donate(later)

        @pl.when(t < units)
        def _():
            pass_on(t)

        for lag, what in zip(
            LAGS, (own_sums, pair_own, merged_sums, pair_merged, trade, exposures, share, products, finish)
        ):
            stage(lag, what)
        return carry

    lax.fori_loop(0, cuts * (days - 1) + LAGS[-1] + 1, turn, 0)

    def drain(d, carry):
        for q in range(cuts):
            u = d * cuts + q
            gather(u, 0, col).wait_send()
            gather(u, 1, col).wait_send()
            gather(u, 2, col).wait_send()
            gather(u, 3, merger(d)).wait_send()
        swap_copy(d).wait_send()
        exp_gather(d, 0, col).wait_send()
        exp_gather(d, 1, col).wait_send()
        exp_gather(d, 2, near_x).wait_send()
        exp_gather(d, 3, near_y).wait_send()
        exp_row_copy(d, mate, row, mate).wait_send()
        for peer in chip_peers():
            exp_row_copy(d, 2 * peer + core, row, 2 * peer + core).wait_send()
            exp_row_copy(d, 2 * peer + 1 - core, 2 * peer + core, mate).wait_send()
        for peer in col_peers():
            prod_copy(d, peer, col).wait_send()

        @pl.when(d >= days - 2)
        def _():
            for lane in range(3):
                mate_copy(d, lane).wait_send()
                for peer in chip_peers():
                    part_copy(d, lane, peer, mine).wait_send()

        return carry

    lax.fori_loop(0, days, drain, 0)


def fused(loadings, weights, specific, factor_cov):
    rows, cols = lax.axis_size("row"), lax.axis_size("col")
    days, assets, factors = loadings.shape
    ports = weights.shape[2]
    slab = ports * cols // rows
    half, wide = assets // 2, 2 * (factors + ports)
    scales = specific.reshape(days, assets // 128, 128)
    anywhere = pl.BlockSpec(memory_space=pl.ANY)
    inside = pl.BlockSpec(memory_space=pltpu.VMEM)
    dma = pltpu.SemaphoreType.DMA
    return pl.pallas_call(
        functools.partial(kernel, rows, cols, CUTS),
        out_shape=jax.ShapeDtypeStruct((days, slab, ports), F32),
        in_specs=[anywhere, anywhere, inside, anywhere],
        out_specs=inside,
        scratch_shapes=[
            pltpu.VMEM((days, cols, half, ports), BF16),
            pltpu.VMEM((2, half, factors), BF16),
            pltpu.VMEM((days, half, factors), BF16),
            pltpu.VMEM((2, factors, cols * factors), F32),
            pltpu.VMEM((half, 2 * ports), BF16),
            pltpu.VMEM((2, 2, rows // 2, slab, wide), F32),
            pltpu.VMEM((days, rows // 2, slab, wide), F32),
            pltpu.VMEM((2, rows // 2, slab, wide), F32),
            pltpu.VMEM((days, rows // 2, slab, wide), F32),
            pltpu.VMEM((days, slab, factors), F32),
            pltpu.VMEM((days, slab, factors), F32),
            pltpu.VMEM((days, cols * ports, factors), F32),
            pltpu.VMEM((days, cols, slab, factors), F32),
            pltpu.VMEM((days, slab, ports), F32),
            pltpu.VMEM((days, cols, slab, ports), F32),
            pltpu.VMEM((days, cols, slab, ports), F32),
            dma((days,)), dma((2,)), dma((2,)),
            dma((days * CUTS, 4)), dma((days * CUTS, 4)),
            dma((days, 3)), dma((days, 3)),
            dma((days, 3, rows // 2)), dma((days, 3, rows // 2)),
            dma((days,)), dma((days,)),
            dma((days, rows)), dma((days, rows)),
            dma((days, 4)), dma((days, 4)),
            dma((days, cols)), dma((days, cols)),
        ],
        compiler_params=pltpu.CompilerParams(
            collective_id=0, has_side_effects=True, vmem_limit_bytes=67_000_000
        ),
        name="covariance",
    )(loadings, weights, scales, factor_cov)


def plain(loadings, weights, specific, factor_cov):
    factor_cols = loadings.shape[2]
    port_cols = weights.shape[2]
    total_ports = port_cols * lax.axis_size("col")
    port_rows = total_ports // lax.axis_size("row")
    row_start = lax.axis_index("row") * port_rows
    weighted = (specific[:, :, None] * weights.astype(F32)).astype(BF16)
    fragment = lax.all_gather(weights, "col", axis=2, tiled=True)
    exposure_part = jnp.einsum("dar,dap->drp", loadings, fragment, preferred_element_type=F32)
    specific_term = jnp.einsum("dak,dap->dkp", weighted, fragment, preferred_element_type=F32)
    joined = jnp.concatenate([exposure_part, specific_term], axis=1)
    exposure = lax.psum(joined[:, :factor_cols, :], "row")
    specific_block = lax.psum_scatter(
        joined[:, factor_cols:, :], "row", scatter_dimension=2, tiled=True
    )
    exposure_rows = lax.dynamic_slice_in_dim(exposure, row_start, port_rows, 2)
    left_part = jnp.einsum("dri,drs->dis", exposure_rows, factor_cov, precision=HIGHEST)
    left = lax.psum(left_part, "col")
    exposure_cols = lax.all_to_all(exposure, "col", split_axis=2, concat_axis=1, tiled=True)
    factor_block = jnp.einsum("dir,drk->dik", left, exposure_cols, precision=HIGHEST)
    return factor_block + jnp.swapaxes(specific_block, 1, 2)


def solution(mesh):
    in_specs = (P(None, "row", "col"), P(None, "row", "col"), P(None, "row"), P(None, "col", None))
    out_specs = P(None, "row", "col")
    rows, cols = mesh.shape["row"], mesh.shape["col"]
    body = fused if cols == 4 and rows % (2 * cols) == 0 else plain
    return jax.shard_map(body, mesh=mesh, in_specs=in_specs, out_specs=out_specs, check_vma=False)
```

```python
import functools

import jax
import jax.numpy as jnp
from jax import lax
from jax.experimental import pallas as pl
from jax.experimental.pallas import tpu as pltpu
from jax.sharding import PartitionSpec as P

F32, BF16 = jnp.float32, jnp.bfloat16
HIGHEST = lax.Precision.HIGHEST
CUTS, AHEAD, EXTRA = 4, 2, 0
LAGS = (4, 5, 5, 6, 9, 11, 13, 16, 19)
GIVEN = (((0, 0), (0, 1), (0, 2)), ((0, 3), (1, 0)), ((1, 1),), ((1, 2), (1, 3)))


def by_dim(a, b, dim, precision=None):
    return lax.dot_general(
        a, b, (((dim,), (dim,)), ((), ())), precision=precision, preferred_element_type=F32
    )


def kernel(
    rows, cols, cuts, load_hbm, weight_hbm, spec_ref, fcov_hbm, out_ref,
    scale_rows, held, load, load_in, fcov, weighted, part, mate_in, pair, part_in, swap, swap_in,
    exp_rows, exp_cols, own_spec, prod, prod_in,
    w_sem, l_sem, f_sem, g_send, g_recv, m_send, m_recv, p_send, p_recv, s_send, s_recv,
    er_send, er_recv, ec_send, ec_recv, q_send, q_recv,
):
    days, assets, factors = load_hbm.shape
    ports = weight_hbm.shape[2]
    slab = ports * cols // rows
    row, col = lax.axis_index("row"), lax.axis_index("col")
    near_x = col + 1 - 2 * (col % 2)
    near_y = (col + 2) % 4
    far = 3 - col
    chips, per = rows // 2, rows // cols
    half = assets // 2
    piece = half // cuts
    mine, core = row // 2, row % 2
    spans = (pl.ds(0, factors), pl.ds(factors, factors), pl.ds(2 * factors, 2 * ports))
    mate = row + 1 - 2 * core

    def merger(d):
        return near_x + (d % 2) * (near_y - near_x)

    def other(d):
        return near_y + (d % 2) * (near_x - near_y)

    def side(d):
        return col % 2 + (d % 2) * (col // 2 - col % 2)

    def to_row(r):
        return {"row": r, "col": col}

    def to_col(c):
        return {"row": row, "col": c}

    def remote(src, dst, send, recv, where):
        return pltpu.make_async_remote_copy(
            src_ref=src, dst_ref=dst, send_sem=send, recv_sem=recv,
            device_id=where, device_id_type=pl.DeviceIdType.MESH,
        )

    def kept(d, start, size):
        return pl.ds(pl.multiple_of(side(d) * half + start, piece), size)

    def given(d, start, size):
        return pl.ds(pl.multiple_of((1 - side(d)) * half + start, piece), size)

    def gather(u, lane, block):
        d, start = u // cuts, pl.multiple_of((u % cuts) * piece, piece)
        if lane == 1:
            dst = load_in.at[d, pl.ds(start, piece)]
            src = load_hbm.at[d, given(d, start, piece)]
        else:
            dst = held.at[d, block, pl.ds(start, piece)]
            src = dst
        if lane == 0:
            src = weight_hbm.at[d, given(d, start, piece)]
        if lane == 2:
            src = weight_hbm.at[d, kept(d, start, piece)]
        where = merger(d) if lane < 2 else other(d)
        return remote(src, dst, g_send.at[u, lane], g_recv.at[u, lane], to_col(where))

    def own_weights(d):
        return pltpu.make_async_copy(
            weight_hbm.at[d, kept(d, 0, half)], held.at[d, col], w_sem.at[d]
        )

    def get_load(d):
        return pltpu.make_async_copy(
            load_hbm.at[d, kept(d, 0, half)], load.at[d % 2], l_sem.at[d % 2]
        )

    def get_fcov(d):
        return pltpu.make_async_copy(fcov_hbm.at[d], fcov.at[d % 2], f_sem.at[d % 2])

    def mate_copy(d, lane):
        span = spans[lane]
        return remote(
            part.at[d % 2, 1 - core, :, :, span], mate_in.at[d, :, :, span],
            m_send.at[d, lane], m_recv.at[d, lane], to_row(mate),
        )

    def part_copy(d, lane, other_chip, landed):
        span = spans[lane]
        return remote(
            pair.at[d % 2, other_chip, :, span], part_in.at[d, landed, :, span],
            p_send.at[d, lane, other_chip], p_recv.at[d, lane, landed],
            to_row(2 * other_chip + core),
        )

    def summed(d, lane):
        for peer in chip_peers():
            part_copy(d, lane, mine, peer).wait_recv()
        total = part_in[d, 0, :, spans[lane]]
        for z in range(1, chips):
            total = total + part_in[d, z, :, spans[lane]]
        return total

    def swap_copy(d):
        return remote(
            swap.at[d], swap_in.at[d], s_send.at[d], s_recv.at[d], to_col(merger(d))
        )

    def exp_gather(d, lane, block):
        start, size = (slab // 2 if lane == 3 else 0), (slab if lane < 2 else slab // 2)
        ref = exp_cols.at[d, block, pl.ds(start, size)]
        where = near_x if lane in (0, 3) else near_y
        return remote(ref, ref, ec_send.at[d, lane], ec_recv.at[d, lane], to_col(where))

    def exp_row_copy(d, slot, landed, other_row):
        ref = exp_rows.at[d, pl.ds(pl.multiple_of(landed * slab, slab), slab)]
        return remote(ref, ref, er_send.at[d, slot], er_recv.at[d, landed], to_row(other_row))

    def prod_copy(d, other_col, landed):
        return remote(
            prod.at[d, other_col], prod_in.at[d, landed],
            q_send.at[d, other_col], q_recv.at[d, landed], to_col(other_col),
        )

    def row_peers():
        return [(row + step) % rows for step in range(1, rows)]

    def chip_peers():
        return [(mine + step) % chips for step in range(1, chips)]

    def col_peers():
        return [near_x, near_y, far]

    def exchange_own(u):
        gather(u, 2, col).start()

    def donate(u):
        first = u - u % cuts
        for q, parts in enumerate(GIVEN):
            @pl.when(u % cuts == q)
            def _(parts=parts):
                for lane, part_of_day in parts:
                    gather(first + part_of_day, lane, col).start()

    def pass_on(u):
        block = merger(u // cuts)

        @pl.when(u % cuts < cuts // 2)
        def _():
            for step in range(2):
                chunk = u + u % cuts + step
                gather(chunk, 0, block).wait_recv()
                gather(chunk, 3, block).start()

    def store(slot, j, lane, values):
        for i in range(per):
            place = j * (per // 2) + i // 2
            part[slot, i % 2, place, :, pl.ds(lane, values.shape[1])] = (
                values[i * slab : (i + 1) * slab]
            )

    def sum_own(d, j):
        slot = d % 2
        lhs = held[d, j]
        store(slot, j, factors, by_dim(lhs, load[slot], 0))
        store(slot, j, 2 * factors, by_dim(lhs, weighted[...], 0))

    def own_sums(d):
        for q in range(cuts):
            gather(d * cuts + q, 2, other(d)).wait_recv()
            gather(d * cuts + q, 3, far).wait_recv()
        own_weights(d).wait()
        groups = half // 128
        scales = scale_rows[d, pl.ds(pl.multiple_of(side(d) * groups, groups), groups)]
        copies = -(-128 // groups)
        tall = jnp.concatenate([scales] * copies, axis=0).T
        for i in range(groups):
            span = pl.ds(i * 128, 128)
            for lane, block in enumerate((col, merger(d))):
                scaled = held[d, block, span].astype(F32) * tall[:, i : i + 1]
                weighted[span, pl.ds(lane * ports, ports)] = scaled.astype(BF16)

        @pl.when(d >= 2)
        def _():
            for lane in range(3):
                mate_copy(d - 2, lane).wait_send()
                for peer in chip_peers():
                    part_copy(d - 2, lane, peer, mine).wait_send()

        get_load(d).wait()

        def own_block(j, carry):
            sum_own(d, j)
            return carry

        lax.fori_loop(0, cols, own_block, 0)
        mate_copy(d, 1).start()
        mate_copy(d, 2).start()

        @pl.when(d + 2 < days)
        def _():
            get_load(d + 2).start()

    def merged_sums(d):
        for q in range(cuts):
            gather(d * cuts + q, 1, col).wait_recv()

        def merged_block(j, carry):
            store(d % 2, j, 0, by_dim(held[d, j], load_in[d], 0))
            return carry

        lax.fori_loop(0, cols, merged_block, 0)
        mate_copy(d, 0).start()

    def pair_up(d, lane):
        slot, span = d % 2, spans[lane]
        mate_copy(d, lane).wait_recv()
        for peer in chip_peers():
            pair[slot, peer, :, span] = part[slot, core, peer, :, span] + mate_in[d, peer, :, span]
            part_copy(d, lane, peer, mine).start()
        part_in[d, mine, :, span] = part[slot, core, mine, :, span] + mate_in[d, mine, :, span]

    def pair_own(d):
        pair_up(d, 1)
        pair_up(d, 2)

    def pair_merged(d):
        pair_up(d, 0)

    def trade(d):
        swap[d] = summed(d, 0)
        swap_copy(d).start()

    def exposures(d):
        total = summed(d, 1)
        swap_copy(d).wait_recv()
        own = total + swap_in[d]
        exp_cols[d, col] = own
        exp_rows[d, pl.ds(pl.multiple_of(row * slab, slab), slab)] = own
        for peer in chip_peers():
            exp_row_copy(d, 2 * peer + core, row, 2 * peer + core).start()
        exp_gather(d, 0, col).start()
        exp_gather(d, 1, col).start()
        exp_row_copy(d, mate, row, mate).start()

    def share(d):
        exp_gather(d, 0, near_x).wait_recv()
        exp_gather(d, 2, near_x).start()
        exp_gather(d, 1, near_y).wait_recv()
        exp_gather(d, 3, near_y).start()
        for peer in chip_peers():
            exp_row_copy(d, row, 2 * peer + core, mate).wait_recv()
            exp_row_copy(d, 2 * peer + 1 - core, 2 * peer + core, mate).start()

    def products(d):
        slot = d % 2
        get_fcov(d).wait()
        exp_gather(d, 2, far).wait_recv()
        exp_gather(d, 3, far).wait_recv()
        left = jnp.zeros((slab, factors), F32)
        for j in range(cols):
            left = left + by_dim(
                exp_cols[d, j], fcov[slot, :, pl.ds(j * factors, factors)], 1, HIGHEST
            )

        @pl.when(d + 2 < days)
        def _():
            get_fcov(d + 2).start()

        def product(j):
            block = exp_rows[d, pl.ds(pl.multiple_of(j * ports, ports), ports)]
            return by_dim(left, block, 1, HIGHEST)

        exp_row_copy(d, row, mate, mate).wait_recv()
        prod[d, mine] = product(mine)
        for peer in chip_peers():
            exp_row_copy(d, row, 2 * peer + 1 - core, mate).wait_recv()
            prod[d, peer] = product(peer)
        total = summed(d, 2)
        own_spec[d] = total[:, :ports]
        block = merger(d)
        prod[d, block] = prod[d, block] + total[:, ports:]
        for peer in col_peers():
            prod_copy(d, peer, col).start()
        prod_in[d, col] = prod[d, col]

    def finish(d):
        for peer in col_peers():
            prod_copy(d, col, peer).wait_recv()
        total = own_spec[d]
        for j in range(cols):
            total = total + prod_in[d, j]
        out_ref[d] = total

    barrier = pltpu.get_barrier_semaphore()
    for peer in row_peers():
        pl.semaphore_signal(
            barrier, inc=1, device_id=to_row(peer), device_id_type=pl.DeviceIdType.MESH
        )
    for peer in col_peers():
        pl.semaphore_signal(
            barrier, inc=1, device_id=to_col(peer), device_id_type=pl.DeviceIdType.MESH
        )
    for d in range(days):
        own_weights(d).start()
    for d in range(min(2, days)):
        get_load(d).start()
        get_fcov(d).start()
    pl.semaphore_wait(barrier, rows + cols - 2)

    units = cuts * days
    for u in range(AHEAD):
        exchange_own(u)
    for u in range(AHEAD + EXTRA):
        if u < AHEAD or (u // cuts) % 2 == 1:
            donate(u)

    for i in range(assets // 128):
        scale_rows[:, i, :] = spec_ref[:, pl.ds(i * 128, 128)]

    def turn(t, carry):
        def stage(lag, what):
            @pl.when((t >= lag) & ((t - lag) % cuts == 0) & (t - lag < units))
            def _():
                what((t - lag) // cuts)

        soon, later = t + AHEAD, t + AHEAD + EXTRA

        @pl.when((soon < units) & ((soon // cuts) % 2 == 0))
        def _():
            donate(soon)

        @pl.when(soon < units)
        def _():
            exchange_own(soon)

        @pl.when((later < units) & ((later // cuts) % 2 == 1))
        def _():
            donate(later)

        @pl.when(t < units)
        def _():
            pass_on(t)

        for lag, what in zip(
            LAGS, (own_sums, pair_own, merged_sums, pair_merged, trade, exposures, share, products, finish)
        ):
            stage(lag, what)
        return carry

    lax.fori_loop(0, cuts * (days - 1) + LAGS[-1] + 1, turn, 0)

    def drain(d, carry):
        for q in range(cuts):
            u = d * cuts + q
            gather(u, 0, col).wait_send()
            gather(u, 1, col).wait_send()
            gather(u, 2, col).wait_send()
            gather(u, 3, merger(d)).wait_send()
        swap_copy(d).wait_send()
        exp_gather(d, 0, col).wait_send()
        exp_gather(d, 1, col).wait_send()
        exp_gather(d, 2, near_x).wait_send()
        exp_gather(d, 3, near_y).wait_send()
        exp_row_copy(d, mate, row, mate).wait_send()
        for peer in chip_peers():
            exp_row_copy(d, 2 * peer + core, row, 2 * peer + core).wait_send()
            exp_row_copy(d, 2 * peer + 1 - core, 2 * peer + core, mate).wait_send()
        for peer in col_peers():
            prod_copy(d, peer, col).wait_send()

        @pl.when(d >= days - 2)
        def _():
            for lane in range(3):
                mate_copy(d, lane).wait_send()
                for peer in chip_peers():
                    part_copy(d, lane, peer, mine).wait_send()

        return carry

    lax.fori_loop(0, days, drain, 0)


def fused(loadings, weights, specific, factor_cov):
    rows, cols = lax.axis_size("row"), lax.axis_size("col")
    days, assets, factors = loadings.shape
    ports = weights.shape[2]
    slab = ports * cols // rows
    half, wide = assets // 2, 2 * (factors + ports)
    anywhere = pl.BlockSpec(memory_space=pl.ANY)
    inside = pl.BlockSpec(memory_space=pltpu.VMEM)
    dma = pltpu.SemaphoreType.DMA
    return pl.pallas_call(
        functools.partial(kernel, rows, cols, CUTS),
        out_shape=jax.ShapeDtypeStruct((days, slab, ports), F32),
        in_specs=[anywhere, anywhere, inside, anywhere],
        out_specs=inside,
        scratch_shapes=[
            pltpu.VMEM((days, assets // 128, 128), F32),
            pltpu.VMEM((days, cols, half, ports), BF16),
            pltpu.VMEM((2, half, factors), BF16),
            pltpu.VMEM((days, half, factors), BF16),
            pltpu.VMEM((2, factors, cols * factors), F32),
            pltpu.VMEM((half, 2 * ports), BF16),
            pltpu.VMEM((2, 2, rows // 2, slab, wide), F32),
            pltpu.VMEM((days, rows // 2, slab, wide), F32),
            pltpu.VMEM((2, rows // 2, slab, wide), F32),
            pltpu.VMEM((days, rows // 2, slab, wide), F32),
            pltpu.VMEM((days, slab, factors), F32),
            pltpu.VMEM((days, slab, factors), F32),
            pltpu.VMEM((days, cols * ports, factors), F32),
            pltpu.VMEM((days, cols, slab, factors), F32),
            pltpu.VMEM((days, slab, ports), F32),
            pltpu.VMEM((days, cols, slab, ports), F32),
            pltpu.VMEM((days, cols, slab, ports), F32),
            dma((days,)), dma((2,)), dma((2,)),
            dma((days * CUTS, 4)), dma((days * CUTS, 4)),
            dma((days, 3)), dma((days, 3)),
            dma((days, 3, rows // 2)), dma((days, 3, rows // 2)),
            dma((days,)), dma((days,)),
            dma((days, rows)), dma((days, rows)),
            dma((days, 4)), dma((days, 4)),
            dma((days, cols)), dma((days, cols)),
        ],
        compiler_params=pltpu.CompilerParams(
            collective_id=0, has_side_effects=True, vmem_limit_bytes=67_000_000
        ),
        name="covariance",
    )(loadings, weights, specific, factor_cov)


def plain(loadings, weights, specific, factor_cov):
    factor_cols = loadings.shape[2]
    port_cols = weights.shape[2]
    total_ports = port_cols * lax.axis_size("col")
    port_rows = total_ports // lax.axis_size("row")
    row_start = lax.axis_index("row") * port_rows
    weighted = (specific[:, :, None] * weights.astype(F32)).astype(BF16)
    fragment = lax.all_gather(weights, "col", axis=2, tiled=True)
    exposure_part = jnp.einsum("dar,dap->drp", loadings, fragment, preferred_element_type=F32)
    specific_term = jnp.einsum("dak,dap->dkp", weighted, fragment, preferred_element_type=F32)
    joined = jnp.concatenate([exposure_part, specific_term], axis=1)
    exposure = lax.psum(joined[:, :factor_cols, :], "row")
    specific_block = lax.psum_scatter(
        joined[:, factor_cols:, :], "row", scatter_dimension=2, tiled=True
    )
    exposure_rows = lax.dynamic_slice_in_dim(exposure, row_start, port_rows, 2)
    left_part = jnp.einsum("dri,drs->dis", exposure_rows, factor_cov, precision=HIGHEST)
    left = lax.psum(left_part, "col")
    exposure_cols = lax.all_to_all(exposure, "col", split_axis=2, concat_axis=1, tiled=True)
    factor_block = jnp.einsum("dir,drk->dik", left, exposure_cols, precision=HIGHEST)
    return factor_block + jnp.swapaxes(specific_block, 1, 2)


def solution(mesh):
    in_specs = (P(None, "row", "col"), P(None, "row", "col"), P(None, "row"), P(None, "col", None))
    out_specs = P(None, "row", "col")
    rows, cols = mesh.shape["row"], mesh.shape["col"]
    body = fused if cols == 4 and rows == 2 * cols else plain
    return jax.shard_map(body, mesh=mesh, in_specs=in_specs, out_specs=out_specs, check_vma=False)
```

```python
import functools

import jax
import jax.numpy as jnp
from jax import lax
from jax.experimental import pallas as pl
from jax.experimental.pallas import tpu as pltpu
from jax.sharding import PartitionSpec as P

F32, BF16 = jnp.float32, jnp.bfloat16
HIGHEST = lax.Precision.HIGHEST
CUTS, AHEAD, EXTRA = 4, 1, 0
LAGS = (4, 5, 5, 6, 8, 10, 12, 14, 16)
GIVEN = (((0, 0), (0, 1), (0, 2)), ((0, 3), (1, 0)), ((1, 1),), ((1, 2), (1, 3)))


def by_dim(a, b, dim, precision=None):
    return lax.dot_general(
        a, b, (((dim,), (dim,)), ((), ())), precision=precision, preferred_element_type=F32
    )


def kernel(
    rows, cols, cuts, load_hbm, weight_hbm, spec_ref, fcov_hbm, out_ref,
    scale_rows, held, load, load_in, fcov, weighted, part, mate_in, pair, part_in, swap, swap_in,
    exp_rows, exp_cols, own_spec, prod, prod_in,
    w_sem, l_sem, f_sem, g_send, g_recv, m_send, m_recv, p_send, p_recv, s_send, s_recv,
    er_send, er_recv, ec_send, ec_recv, q_send, q_recv,
):
    days, assets, factors = load_hbm.shape
    ports = weight_hbm.shape[2]
    slab = ports * cols // rows
    row, col = lax.axis_index("row"), lax.axis_index("col")
    near_x = col + 1 - 2 * (col % 2)
    near_y = (col + 2) % 4
    far = 3 - col
    chips, per = rows // 2, rows // cols
    half = assets // 2
    piece = half // cuts
    mine, core = row // 2, row % 2
    spans = (pl.ds(0, factors), pl.ds(factors, factors), pl.ds(2 * factors, 2 * ports))
    mate = row + 1 - 2 * core

    def merger(d):
        return near_x + (d % 2) * (near_y - near_x)

    def other(d):
        return near_y + (d % 2) * (near_x - near_y)

    def side(d):
        return col % 2 + (d % 2) * (col // 2 - col % 2)

    def to_row(r):
        return {"row": r, "col": col}

    def to_col(c):
        return {"row": row, "col": c}

    def remote(src, dst, send, recv, where):
        return pltpu.make_async_remote_copy(
            src_ref=src, dst_ref=dst, send_sem=send, recv_sem=recv,
            device_id=where, device_id_type=pl.DeviceIdType.MESH,
        )

    def kept(d, start, size):
        return pl.ds(pl.multiple_of(side(d) * half + start, piece), size)

    def given(d, start, size):
        return pl.ds(pl.multiple_of((1 - side(d)) * half + start, piece), size)

    def gather(u, lane, block):
        d, start = u // cuts, pl.multiple_of((u % cuts) * piece, piece)
        if lane == 1:
            dst = load_in.at[d, pl.ds(start, piece)]
            src = load_hbm.at[d, given(d, start, piece)]
        else:
            dst = held.at[d, block, pl.ds(start, piece)]
            src = dst
        if lane == 0:
            src = weight_hbm.at[d, given(d, start, piece)]
        if lane == 2:
            src = weight_hbm.at[d, kept(d, start, piece)]
        where = merger(d) if lane < 2 else other(d)
        return remote(src, dst, g_send.at[u, lane], g_recv.at[u, lane], to_col(where))

    def own_weights(d):
        return pltpu.make_async_copy(
            weight_hbm.at[d, kept(d, 0, half)], held.at[d, col], w_sem.at[d]
        )

    def get_load(d):
        return pltpu.make_async_copy(
            load_hbm.at[d, kept(d, 0, half)], load.at[d % 2], l_sem.at[d % 2]
        )

    def get_fcov(d):
        return pltpu.make_async_copy(fcov_hbm.at[d], fcov.at[d % 2], f_sem.at[d % 2])

    def mate_copy(d, lane):
        span = spans[lane]
        return remote(
            part.at[d % 2, 1 - core, :, :, span], mate_in.at[d, :, :, span],
            m_send.at[d, lane], m_recv.at[d, lane], to_row(mate),
        )

    def part_copy(d, lane, other_chip, landed):
        span = spans[lane]
        return remote(
            pair.at[d % 2, other_chip, :, span], part_in.at[d, landed, :, span],
            p_send.at[d, lane, other_chip], p_recv.at[d, lane, landed],
            to_row(2 * other_chip + core),
        )

    def summed(d, lane):
        for peer in chip_peers():
            part_copy(d, lane, mine, peer).wait_recv()
        total = part_in[d, 0, :, spans[lane]]
        for z in range(1, chips):
            total = total + part_in[d, z, :, spans[lane]]
        return total

    def swap_copy(d):
        return remote(
            swap.at[d], swap_in.at[d], s_send.at[d], s_recv.at[d], to_col(merger(d))
        )

    def exp_gather(d, lane, block):
        start, size = (slab // 2 if lane == 3 else 0), (slab if lane < 2 else slab // 2)
        ref = exp_cols.at[d, block, pl.ds(start, size)]
        where = near_x if lane in (0, 3) else near_y
        return remote(ref, ref, ec_send.at[d, lane], ec_recv.at[d, lane], to_col(where))

    def exp_row_copy(d, slot, landed, other_row):
        ref = exp_rows.at[d, pl.ds(pl.multiple_of(landed * slab, slab), slab)]
        return remote(ref, ref, er_send.at[d, slot], er_recv.at[d, landed], to_row(other_row))

    def prod_copy(d, other_col, landed):
        return remote(
            prod.at[d, other_col], prod_in.at[d, landed],
            q_send.at[d, other_col], q_recv.at[d, landed], to_col(other_col),
        )

    def row_peers():
        return [(row + step) % rows for step in range(1, rows)]

    def chip_peers():
        return [(mine + step) % chips for step in range(1, chips)]

    def col_peers():
        return [near_x, near_y, far]

    def exchange_own(u):
        gather(u, 2, col).start()

    def donate(u):
        first = u - u % cuts
        for q, parts in enumerate(GIVEN):
            @pl.when(u % cuts == q)
            def _(parts=parts):
                for lane, part_of_day in parts:
                    gather(first + part_of_day, lane, col).start()

    def pass_on(u):
        block = merger(u // cuts)

        @pl.when(u % cuts < cuts // 2)
        def _():
            for step in range(2):
                chunk = u + u % cuts + step
                gather(chunk, 0, block).wait_recv()
                gather(chunk, 3, block).start()

    def store(slot, j, lane, values):
        for i in range(per):
            place = j * (per // 2) + i // 2
            part[slot, i % 2, place, :, pl.ds(lane, values.shape[1])] = (
                values[i * slab : (i + 1) * slab]
            )

    def sum_own(d, j):
        slot = d % 2
        lhs = held[d, j]
        store(slot, j, factors, by_dim(lhs, load[slot], 0))
        store(slot, j, 2 * factors, by_dim(lhs, weighted[...], 0))

    def own_sums(d):
        for q in range(cuts):
            gather(d * cuts + q, 2, other(d)).wait_recv()
            gather(d * cuts + q, 3, far).wait_recv()
        own_weights(d).wait()
        groups = half // 128
        scales = scale_rows[d, pl.ds(pl.multiple_of(side(d) * groups, groups), groups)]
        copies = -(-128 // groups)
        tall = jnp.concatenate([scales] * copies, axis=0).T
        for i in range(groups):
            span = pl.ds(i * 128, 128)
            for lane, block in enumerate((col, merger(d))):
                scaled = held[d, block, span].astype(F32) * tall[:, i : i + 1]
                weighted[span, pl.ds(lane * ports, ports)] = scaled.astype(BF16)

        @pl.when(d >= 2)
        def _():
            for lane in range(3):
                mate_copy(d - 2, lane).wait_send()
                for peer in chip_peers():
                    part_copy(d - 2, lane, peer, mine).wait_send()

        get_load(d).wait()

        def own_block(j, carry):
            sum_own(d, j)
            return carry

        lax.fori_loop(0, cols, own_block, 0)
        mate_copy(d, 1).start()
        mate_copy(d, 2).start()

        @pl.when(d + 2 < days)
        def _():
            get_load(d + 2).start()

    def merged_sums(d):
        for q in range(cuts):
            gather(d * cuts + q, 1, col).wait_recv()

        def merged_block(j, carry):
            store(d % 2, j, 0, by_dim(held[d, j], load_in[d], 0))
            return carry

        lax.fori_loop(0, cols, merged_block, 0)
        mate_copy(d, 0).start()

    def pair_up(d, lane):
        slot, span = d % 2, spans[lane]
        mate_copy(d, lane).wait_recv()
        for peer in chip_peers():
            pair[slot, peer, :, span] = part[slot, core, peer, :, span] + mate_in[d, peer, :, span]
            part_copy(d, lane, peer, mine).start()
        part_in[d, mine, :, span] = part[slot, core, mine, :, span] + mate_in[d, mine, :, span]

    def pair_own(d):
        pair_up(d, 1)
        pair_up(d, 2)

    def pair_merged(d):
        pair_up(d, 0)

    def trade(d):
        swap[d] = summed(d, 0)
        swap_copy(d).start()

    def exposures(d):
        total = summed(d, 1)
        swap_copy(d).wait_recv()
        own = total + swap_in[d]
        exp_cols[d, col] = own
        exp_rows[d, pl.ds(pl.multiple_of(row * slab, slab), slab)] = own
        for peer in chip_peers():
            exp_row_copy(d, 2 * peer + core, row, 2 * peer + core).start()
        exp_gather(d, 0, col).start()
        exp_gather(d, 1, col).start()
        exp_row_copy(d, mate, row, mate).start()

    def share(d):
        exp_gather(d, 0, near_x).wait_recv()
        exp_gather(d, 2, near_x).start()
        exp_gather(d, 1, near_y).wait_recv()
        exp_gather(d, 3, near_y).start()
        for peer in chip_peers():
            exp_row_copy(d, row, 2 * peer + core, mate).wait_recv()
            exp_row_copy(d, 2 * peer + 1 - core, 2 * peer + core, mate).start()

    def products(d):
        slot = d % 2
        get_fcov(d).wait()
        exp_gather(d, 2, far).wait_recv()
        exp_gather(d, 3, far).wait_recv()
        left = jnp.zeros((slab, factors), F32)
        for j in range(cols):
            left = left + by_dim(
                exp_cols[d, j], fcov[slot, :, pl.ds(j * factors, factors)], 1, HIGHEST
            )

        @pl.when(d + 2 < days)
        def _():
            get_fcov(d + 2).start()

        def product(j):
            block = exp_rows[d, pl.ds(pl.multiple_of(j * ports, ports), ports)]
            return by_dim(left, block, 1, HIGHEST)

        exp_row_copy(d, row, mate, mate).wait_recv()
        prod[d, mine] = product(mine)
        for peer in chip_peers():
            exp_row_copy(d, row, 2 * peer + 1 - core, mate).wait_recv()
            prod[d, peer] = product(peer)
        total = summed(d, 2)
        own_spec[d] = total[:, :ports]
        block = merger(d)
        prod[d, block] = prod[d, block] + total[:, ports:]
        for peer in col_peers():
            prod_copy(d, peer, col).start()
        prod_in[d, col] = prod[d, col]

    def finish(d):
        for peer in col_peers():
            prod_copy(d, col, peer).wait_recv()
        total = own_spec[d]
        for j in range(cols):
            total = total + prod_in[d, j]
        out_ref[d] = total

    barrier = pltpu.get_barrier_semaphore()
    for peer in row_peers():
        pl.semaphore_signal(
            barrier, inc=1, device_id=to_row(peer), device_id_type=pl.DeviceIdType.MESH
        )
    for peer in col_peers():
        pl.semaphore_signal(
            barrier, inc=1, device_id=to_col(peer), device_id_type=pl.DeviceIdType.MESH
        )
    for d in range(days):
        own_weights(d).start()
    for d in range(min(2, days)):
        get_load(d).start()
        get_fcov(d).start()
    pl.semaphore_wait(barrier, rows + cols - 2)

    units = cuts * days
    for u in range(AHEAD):
        exchange_own(u)
    for u in range(AHEAD + EXTRA):
        if u < AHEAD or (u // cuts) % 2 == 1:
            donate(u)

    for i in range(assets // 128):
        scale_rows[:, i, :] = spec_ref[:, pl.ds(i * 128, 128)]

    def turn(t, carry):
        def stage(lag, what):
            @pl.when((t >= lag) & ((t - lag) % cuts == 0) & (t - lag < units))
            def _():
                what((t - lag) // cuts)

        soon, later = t + AHEAD, t + AHEAD + EXTRA

        @pl.when((soon < units) & ((soon // cuts) % 2 == 0))
        def _():
            donate(soon)

        @pl.when(soon < units)
        def _():
            exchange_own(soon)

        @pl.when((later < units) & ((later // cuts) % 2 == 1))
        def _():
            donate(later)

        @pl.when(t < units)
        def _():
            pass_on(t)

        for lag, what in zip(
            LAGS, (own_sums, pair_own, merged_sums, pair_merged, trade, exposures, share, products, finish)
        ):
            stage(lag, what)
        return carry

    lax.fori_loop(0, cuts * (days - 1) + LAGS[-1] + 1, turn, 0)

    def drain(d, carry):
        for q in range(cuts):
            u = d * cuts + q
            gather(u, 0, col).wait_send()
            gather(u, 1, col).wait_send()
            gather(u, 2, col).wait_send()
            gather(u, 3, merger(d)).wait_send()
        swap_copy(d).wait_send()
        exp_gather(d, 0, col).wait_send()
        exp_gather(d, 1, col).wait_send()
        exp_gather(d, 2, near_x).wait_send()
        exp_gather(d, 3, near_y).wait_send()
        exp_row_copy(d, mate, row, mate).wait_send()
        for peer in chip_peers():
            exp_row_copy(d, 2 * peer + core, row, 2 * peer + core).wait_send()
            exp_row_copy(d, 2 * peer + 1 - core, 2 * peer + core, mate).wait_send()
        for peer in col_peers():
            prod_copy(d, peer, col).wait_send()

        @pl.when(d >= days - 2)
        def _():
            for lane in range(3):
                mate_copy(d, lane).wait_send()
                for peer in chip_peers():
                    part_copy(d, lane, peer, mine).wait_send()

        return carry

    lax.fori_loop(0, days, drain, 0)


def fused(loadings, weights, specific, factor_cov):
    rows, cols = lax.axis_size("row"), lax.axis_size("col")
    days, assets, factors = loadings.shape
    ports = weights.shape[2]
    slab = ports * cols // rows
    half, wide = assets // 2, 2 * (factors + ports)
    anywhere = pl.BlockSpec(memory_space=pl.ANY)
    inside = pl.BlockSpec(memory_space=pltpu.VMEM)
    dma = pltpu.SemaphoreType.DMA
    return pl.pallas_call(
        functools.partial(kernel, rows, cols, CUTS),
        out_shape=jax.ShapeDtypeStruct((days, slab, ports), F32),
        in_specs=[anywhere, anywhere, inside, anywhere],
        out_specs=inside,
        scratch_shapes=[
            pltpu.VMEM((days, assets // 128, 128), F32),
            pltpu.VMEM((days, cols, half, ports), BF16),
            pltpu.VMEM((2, half, factors), BF16),
            pltpu.VMEM((days, half, factors), BF16),
            pltpu.VMEM((2, factors, cols * factors), F32),
            pltpu.VMEM((half, 2 * ports), BF16),
            pltpu.VMEM((2, 2, rows // 2, slab, wide), F32),
            pltpu.VMEM((days, rows // 2, slab, wide), F32),
            pltpu.VMEM((2, rows // 2, slab, wide), F32),
            pltpu.VMEM((days, rows // 2, slab, wide), F32),
            pltpu.VMEM((days, slab, factors), F32),
            pltpu.VMEM((days, slab, factors), F32),
            pltpu.VMEM((days, cols * ports, factors), F32),
            pltpu.VMEM((days, cols, slab, factors), F32),
            pltpu.VMEM((days, slab, ports), F32),
            pltpu.VMEM((days, cols, slab, ports), F32),
            pltpu.VMEM((days, cols, slab, ports), F32),
            dma((days,)), dma((2,)), dma((2,)),
            dma((days * CUTS, 4)), dma((days * CUTS, 4)),
            dma((days, 3)), dma((days, 3)),
            dma((days, 3, rows // 2)), dma((days, 3, rows // 2)),
            dma((days,)), dma((days,)),
            dma((days, rows)), dma((days, rows)),
            dma((days, 4)), dma((days, 4)),
            dma((days, cols)), dma((days, cols)),
        ],
        compiler_params=pltpu.CompilerParams(
            collective_id=0, has_side_effects=True, vmem_limit_bytes=67_000_000
        ),
        name="covariance",
    )(loadings, weights, specific, factor_cov)


def plain(loadings, weights, specific, factor_cov):
    factor_cols = loadings.shape[2]
    port_cols = weights.shape[2]
    total_ports = port_cols * lax.axis_size("col")
    port_rows = total_ports // lax.axis_size("row")
    row_start = lax.axis_index("row") * port_rows
    weighted = (specific[:, :, None] * weights.astype(F32)).astype(BF16)
    fragment = lax.all_gather(weights, "col", axis=2, tiled=True)
    exposure_part = jnp.einsum("dar,dap->drp", loadings, fragment, preferred_element_type=F32)
    specific_term = jnp.einsum("dak,dap->dkp", weighted, fragment, preferred_element_type=F32)
    joined = jnp.concatenate([exposure_part, specific_term], axis=1)
    exposure = lax.psum(joined[:, :factor_cols, :], "row")
    specific_block = lax.psum_scatter(
        joined[:, factor_cols:, :], "row", scatter_dimension=2, tiled=True
    )
    exposure_rows = lax.dynamic_slice_in_dim(exposure, row_start, port_rows, 2)
    left_part = jnp.einsum("dri,drs->dis", exposure_rows, factor_cov, precision=HIGHEST)
    left = lax.psum(left_part, "col")
    exposure_cols = lax.all_to_all(exposure, "col", split_axis=2, concat_axis=1, tiled=True)
    factor_block = jnp.einsum("dir,drk->dik", left, exposure_cols, precision=HIGHEST)
    return factor_block + jnp.swapaxes(specific_block, 1, 2)


def solution(mesh):
    in_specs = (P(None, "row", "col"), P(None, "row", "col"), P(None, "row"), P(None, "col", None))
    out_specs = P(None, "row", "col")
    rows, cols = mesh.shape["row"], mesh.shape["col"]
    body = fused if cols == 4 and rows == 2 * cols else plain
    return jax.shard_map(body, mesh=mesh, in_specs=in_specs, out_specs=out_specs, check_vma=False)
```
